256 devices in a mesh: groups: 4 (over y, x), ctx: 32 (over z), tp: 2 (over core).
Axes of the slice: x: 2, y: 2, z: 32, core: 2. Of those that a mesh axis runs over, the one named last changes fastest.
The devices are a block of a 4x8x32 slice.
Arguments:
- query_states: bfloat16 [32768, 32, 128], P(('groups', 'ctx'), 'tp'), parts along dimension 0, may hold values from -8 to 8
- key_states: bfloat16 [32768, 4, 128], P(('groups', 'ctx'), 'tp'), parts along dimension 0, may hold values from -8 to 8
- value_rows: bfloat16 [32768, 4, 128], P(('groups', 'ctx'), 'tp'), parts along dimension 0, may hold values from -12 to 12
- positions: int32 [32768], P(('groups', 'ctx')), parts along dimension 0, may hold values from 0 to 8191, as said below
- out_weight: bfloat16 [4096, 4096], P('tp', 'ctx'), may hold values from -0.375 to 0.375
Outputs:
- projected: bfloat16 [32768, 4096], P(('groups', 'ctx'), 'tp'), parts along dimension 0
The draws below stay inside these ranges and needn't reach their ends.
There are 4 independent parts, one for each index of `groups`. The reference program is written for one: setup_inputs(seed, part) draws one part's arguments, and reference() takes and returns one part's arrays. A program takes and returns all parts, laid end to end along the dimension named above; an argument that names none is the same for every part. Nothing has to cross between parts.
Inputs may be any that keep to these rules, and one draw needn't show every extreme that they name: Each of 0 to 8191 appears once. Half-block b holds positions b * 128 to (b + 1) * 128 - 1. The 256 rows of one device along ctx hold half-block j and then half-block 64 - 1 - j, each in rising order, for a j below 32 that differs from device to device.
All inputs are finite; a program needn't handle non-finite values.
Results may differ from the reference program's by a relative error of at most 0.01.
Values may be sent and summed in bfloat16 or wider, within the bound.
A program may use at most 64 MiB of HBM per device.

```python
from functools import partial
import jax
import jax.numpy as jnp
from jax import lax

QUERY_HEAD_COUNT = 32
KEY_VALUE_HEADS = 4
HEAD_WIDTH = 128
DOUT = 4096
HALF = 128
SEQUENCE_LENGTH = 8192
HALF_BLOCK_COUNT = 64


def draw_query_states(key, part):
    base_point = jax.random.fold_in(key, 21)
    value_entries = jnp.clip(jax.random.normal(jax.random.fold_in(base_point, 1), (SEQUENCE_LENGTH, QUERY_HEAD_COUNT, HEAD_WIDTH)), -8.0, 8.0)
    return value_entries.astype(jnp.bfloat16)


def draw_key_states(key, part):
    base_point = jax.random.fold_in(key, 41)
    value_entries = jnp.clip(jax.random.normal(jax.random.fold_in(base_point, 1), (SEQUENCE_LENGTH, KEY_VALUE_HEADS, HEAD_WIDTH)), -8.0, 8.0)
    return value_entries.astype(jnp.bfloat16)


def draw_positions(key, part):
    order = jax.random.permutation(jax.random.fold_in(key, 31), HALF_BLOCK_COUNT // 2)
    within = jnp.arange(HALF)
    lower = order[:, None] * HALF + within[None, :]
    upper = (HALF_BLOCK_COUNT - 1 - order)[:, None] * HALF + within[None, :]
    return jnp.concatenate([lower, upper], axis=1).reshape(SEQUENCE_LENGTH).astype(jnp.int32)


def steps_of(stream_key, dims, cuts, low, top_value):
    loudness = 1.0
    for dim, parts in cuts:
        steps = jax.random.uniform(jax.random.fold_in(jax.random.fold_in(stream_key, 6), dim), (parts,), jnp.float32, low / len(cuts), top_value / len(cuts))
        loudness = loudness * jnp.repeat(jnp.exp(steps), dims[dim] // parts).reshape((-1,) + (1,) * (len(dims) - 1 - dim))
    return loudness


def gaussian(key, shape, scale, limit, shards=(), dtype=jnp.bfloat16):
    loudness = steps_of(key, shape, shards, -0.22, 0.18) if shards else 1.0
    values = jax.random.normal(key, shape, jnp.float32) * scale * loudness
    return jnp.minimum(jnp.maximum(values, -limit), limit).astype(dtype)


def setup_inputs(seed: int = 0, part: int = 0) -> dict:
    streams_of = jax.random.split(jax.random.key(seed), 6)
    part_splits = jax.random.split(jax.random.fold_in(streams_of[5], part), 6)
    query_states = draw_query_states(jax.random.fold_in(jax.random.fold_in(streams_of[5], part), 71), part)
    key_states = draw_key_states(jax.random.fold_in(jax.random.fold_in(streams_of[5], part), 71), part)
    value_rows = gaussian(part_splits[2], (SEQUENCE_LENGTH, KEY_VALUE_HEADS, HEAD_WIDTH), 2.0, 12.0, ((0, 32), (1, 2)))
    positions = draw_positions(jax.random.fold_in(jax.random.fold_in(streams_of[5], part), 71), part)
    out_weight = gaussian(streams_of[4], (QUERY_HEAD_COUNT * HEAD_WIDTH, DOUT), (QUERY_HEAD_COUNT * HEAD_WIDTH // 16) ** -0.5, 0.375, ((0, 2), (1, 32)))
    return {"query_states": query_states, "key_states": key_states, "value_rows": value_rows, "positions": positions, "out_weight": out_weight}


def one_head(operands, visible):
    query_head, key_head, value_head = operands
    scores = jnp.dot(query_head, key_head.T, preferred_element_type=jnp.float32) * (HEAD_WIDTH ** -0.5)
    scores = jnp.where(visible, scores, -jnp.inf)
    largest = jnp.max(scores, axis=1)
    exp_scores = jnp.exp(scores - largest[:, None])
    denominator = jnp.sum(exp_scores, axis=1)
    weighted = jnp.dot(exp_scores.astype(jnp.bfloat16), value_head, preferred_element_type=jnp.float32)
    return (weighted / denominator[:, None]).astype(jnp.bfloat16)


def reference(query_states, key_states, value_rows, positions, out_weight):
    visible = positions[None, :] <= positions[:, None]
    group_width = QUERY_HEAD_COUNT // KEY_VALUE_HEADS
    query_major = jnp.moveaxis(query_states, 1, 0)
    key_major = jnp.repeat(jnp.moveaxis(key_states, 1, 0), group_width, axis=0)
    value_major = jnp.repeat(jnp.moveaxis(value_rows, 1, 0), group_width, axis=0)
    attended = lax.map(partial(one_head, visible=visible), (query_major, key_major, value_major))
    attended = jnp.moveaxis(attended, 0, 1).reshape(SEQUENCE_LENGTH, QUERY_HEAD_COUNT * HEAD_WIDTH)
    return jnp.dot(attended, out_weight, preferred_element_type=jnp.float32).astype(jnp.bfloat16)
```

```python
import functools

import jax
import jax.numpy as jnp
from jax import lax
from jax.experimental import pallas as pl
from jax.experimental.pallas import tpu as pltpu
from jax.sharding import PartitionSpec as P

MESH = pl.DeviceIdType.MESH
LOG2E = 1.4426950408889634
LOW = -1e30
HIGH = 1e30
TAG_ROWS = 16
LANES = 256


def flip(index, stride):
    return index + stride * (1 - 2 * lax.rem(index // stride, 2))


def kernel(
    n, row_stride, kv_heads, half, q_hbm, k_hbm, v_hbm, w_hbm, out_ref,
    q_ref, kbuf, vbuf, wbuf, acc_ref, max_ref, sum_ref, att_ref, give_ref, take_ref,
    in_sem, k_send, v_send, w_send, x_send, y_send, xd_send, yd_send,
    k_recv, v_recv, w_recv, w_last_recv, x_recv, y_recv, xd_recv, yd_recv, give_send, take_recv,
):
    me, group, core = (lax.axis_index(a) for a in ("ctx", "groups", "tp"))
    head_size = q_ref.shape[2]
    width = q_ref.shape[3]
    chunks = width // LANES
    keys = 2 * half
    scale = LOG2E * head_size ** (-0.5)
    rows = wbuf.shape[1]
    quarter, eighth = rows // 4, rows // 8
    steps = n // 2

    right, left = lax.rem(me + 1, n), lax.rem(me + n - 1, n)
    x_group, y_group = flip(group, 1), flip(group, row_stride)
    px, py = lax.rem(group, 2), lax.rem(group // row_stride, 2)
    mine = pl.multiple_of((2 * py + px) * quarter, quarter)
    of_x = pl.multiple_of((2 * py + 1 - px) * quarter, quarter)
    of_y = pl.multiple_of((2 * (1 - py) + px) * quarter, quarter)
    of_xy = pl.multiple_of((2 * (1 - py) + 1 - px) * quarter, quarter)
    to_right, to_left = {"ctx": right}, {"ctx": left}
    to_x, to_y, to_twin = {"groups": x_group}, {"groups": y_group}, {"tp": 1 - core}

    def remote(ref, send, recv, device):
        return pltpu.make_async_remote_copy(
            src_ref=ref, dst_ref=ref, send_sem=send, recv_sem=recv, device_id=device, device_id_type=MESH
        )

    def way(d):
        return to_right if d == 0 else to_left

    def k_copy(d, slot):
        return remote(kbuf.at[slot], k_send.at[d, slot], k_recv.at[slot], way(d))

    def v_copy(d, slot):
        return remote(vbuf.at[slot], v_send.at[d, slot], v_recv.at[slot], way(d))

    def w_copy(d, slot):
        return remote(wbuf.at[slot, pl.ds(mine, quarter)], w_send.at[d, slot], w_recv.at[slot], way(d))

    def w_last_copy(d, slot):
        ref = wbuf.at[slot, pl.ds(mine + d * eighth, eighth)]
        return remote(ref, w_send.at[d, slot], w_recv.at[slot] if d == 0 else w_last_recv.at[0], way(d))

    def x_copy(slot, start):
        return remote(wbuf.at[slot, pl.ds(start, quarter)], x_send.at[slot], x_recv.at[slot], to_x)

    def y_copy(slot, start):
        return remote(wbuf.at[slot, pl.ds(start, quarter)], y_send.at[slot], y_recv.at[slot], to_y)

    def xd_copy(slot, start):
        return remote(wbuf.at[slot, pl.ds(start, eighth)], xd_send.at[slot], xd_recv.at[slot], to_x)

    def yd_copy(slot, start):
        return remote(wbuf.at[slot, pl.ds(start + eighth, eighth)], yd_send.at[slot], yd_recv.at[slot], to_y)

    def side(slot):
        x_copy(slot, mine).start()
        y_copy(slot, mine).start()

    def relay(slot):
        x_copy(slot, of_x).wait_recv()
        yd_copy(slot, of_x).start()
        y_copy(slot, of_y).wait_recv()
        xd_copy(slot, of_y).start()

    own = (
        pltpu.make_async_copy(k_hbm, kbuf.at[me], in_sem.at[0]),
        pltpu.make_async_copy(v_hbm, vbuf.at[me], in_sem.at[1]),
        pltpu.make_async_copy(w_hbm, wbuf.at[me], in_sem.at[2]),
        pltpu.make_async_copy(q_hbm, q_ref, in_sem.at[3]),
    )
    for copy in own:
        copy.start()

    barrier = pltpu.get_barrier_semaphore()
    for device in (to_right, to_left, to_x, to_y, to_twin):
        pl.semaphore_signal(barrier, inc=1, device_id=device, device_id_type=MESH)
    pl.semaphore_wait(barrier, 5)

    own[0].wait()
    for d in (0, 1):
        k_copy(d, me).start()
    own[1].wait()
    for d in (0, 1):
        v_copy(d, me).start()
    own[2].wait()
    for d in (0, 1):
        w_copy(d, me).start()
    own[3].wait()

    def places(i):
        kv = i // chunks
        return kv, pl.ds(pl.multiple_of(lax.rem(i, chunks) * LANES, LANES), LANES)

    def scores_of(key_part, kv, part, lanes):
        return jnp.dot(key_part, q_ref[kv, part, :, lanes], preferred_element_type=jnp.float32)

    def powers(scores, shift):
        return jnp.exp2((scores - shift) * scale)

    def column_max(scores):
        return jnp.max(scores, axis=0, keepdims=True)

    def column_sum(values):
        return jnp.sum(values, axis=0, keepdims=True)

    def first(i, _):
        kv, lanes = places(i)
        key_rows = pl.multiple_of(kv * keys, keys)
        key_block = kbuf[me, pl.ds(key_rows, keys), :]
        values = vbuf[me, kv]
        shape = (half, LANES)
        tri = lax.broadcasted_iota(jnp.int32, shape, 0) <= lax.rem(lax.broadcasted_iota(jnp.int32, shape, 1), half)
        for part in (0, 1):
            scores = scores_of(key_block[: half * (part + 1)], kv, part, lanes)
            pieces = [scores[half * j : half * (j + 1)] for j in range(part + 1)]
            pieces[part] = jnp.where(tri, pieces[part], LOW)
            largest = functools.reduce(jnp.maximum, [column_max(p) for p in pieces])
            exps = jnp.concatenate([powers(p, largest) for p in pieces], axis=0)
            max_ref[kv, part, :, lanes] = largest
            sum_ref[kv, part, :, lanes] = column_sum(exps)
            acc_ref[kv, part, :, lanes] = jnp.dot(
                values[:, : half * (part + 1)], exps.astype(jnp.bfloat16), preferred_element_type=jnp.float32
            )
        return 0

    lax.fori_loop(0, kv_heads * chunks, first, 0)

    def tag(slot):
        row = kbuf[slot, kv_heads * keys :, :].astype(jnp.float32)[:1]
        return jnp.concatenate([row] * (LANES // row.shape[1]), axis=1)

    def attend(slot):
        theirs, ours = tag(slot), tag(me)
        before, after = theirs < ours, theirs > ours

        def one(i, _):
            kv, lanes = places(i)
            key_rows = pl.multiple_of(kv * keys, keys)
            key_block = kbuf[slot, pl.ds(key_rows, keys), :]
            values = vbuf[slot, kv]

            def renew(part, largest, shifts, pieces, value_part):
                old = max_ref[kv, part, :, lanes]
                factor = jnp.exp2((old - largest) * scale)
                exps = jnp.concatenate([powers(p, s) for p, s in zip(pieces, shifts)], axis=0)
                max_ref[kv, part, :, lanes] = largest
                sum_ref[kv, part, :, lanes] = sum_ref[kv, part, :, lanes] * factor + column_sum(exps)
                acc_ref[kv, part, :, lanes] = acc_ref[kv, part, :, lanes] * factor + jnp.dot(
                    value_part, exps.astype(jnp.bfloat16), preferred_element_type=jnp.float32
                )

            low = scores_of(key_block[:half], kv, 0, lanes)
            largest = jnp.maximum(max_ref[kv, 0, :, lanes], jnp.where(before, column_max(low), LOW))
            renew(0, largest, [jnp.where(before, largest, HIGH)], [low], values[:, :half])

            high = scores_of(key_block, kv, 1, lanes)
            pieces = [high[:half], high[half:]]
            largest = jnp.maximum(column_max(pieces[0]), jnp.where(after, column_max(pieces[1]), LOW))
            largest = jnp.maximum(max_ref[kv, 1, :, lanes], largest)
            renew(1, largest, [largest, jnp.where(after, largest, HIGH)], pieces, values)
            return 0

        lax.fori_loop(0, kv_heads * chunks, one, 0)

    def behind(s):
        return lax.rem(me + n - s, n)

    def ahead(s):
        return lax.rem(me + s, n)

    def step(s, _):
        a, b = behind(s), ahead(s)
        k_copy(0, a).wait_recv()
        k_copy(0, a).start()
        k_copy(1, b).wait_recv()

        @pl.when(s < steps - 1)
        def _():
            k_copy(1, b).start()

        v_copy(0, a).wait_recv()

        @pl.when(s < steps - 1)
        def _():
            v_copy(0, a).start()

        v_copy(1, b).wait_recv()
        v_copy(1, b).start()
        attend(a)

        w_copy(0, a).wait_recv()
        w_copy(1, b).wait_recv()

        @pl.when(s < steps - 1)
        def _():
            w_copy(0, a).start()
            w_copy(1, b).start()

        @pl.when(s == steps - 1)
        def _():
            w_last_copy(0, a).start()
            w_last_copy(1, b).start()

        side(a)
        side(b)

        @pl.when(s > 1)
        def _():
            relay(behind(s - 1))
            relay(ahead(s - 1))

        attend(b)
        return 0

    lax.fori_loop(1, steps, step, 0)

    far = ahead(steps)
    k_copy(0, far).wait_recv()
    v_copy(1, far).wait_recv()
    relay(behind(steps - 1))
    relay(ahead(steps - 1))
    attend(far)
    w_last_copy(0, far).wait_recv()
    w_last_copy(1, far).wait_recv()
    side(far)

    heads = width // half

    def finish(i, _):
        kv, part = i // 2, lax.rem(i, 2)
        for h in range(heads):
            lanes = slice(h * half, (h + 1) * half)
            tile = acc_ref[kv, part, :, lanes] / sum_ref[kv, part, :, lanes]
            columns = pl.ds(pl.multiple_of((kv * heads + h) * head_size, head_size), head_size)
            att_ref[pl.ds(pl.multiple_of(part * half, half), half), columns] = tile.T.astype(jnp.bfloat16)
        return 0

    lax.fori_loop(0, kv_heads * 2, finish, 0)

    relay(far)

    def arrived(s, _):
        slot = ahead(s)
        xd_copy(slot, of_xy).wait_recv()
        yd_copy(slot, of_xy).wait_recv()
        return 0

    lax.fori_loop(1, n, arrived, 0)

    pairs = n // 4

    def product(pair):
        weight = jnp.concatenate([wbuf[2 * pair], wbuf[2 * pair + 1]], axis=1)
        return jnp.dot(att_ref[...], weight, preferred_element_type=jnp.float32)

    def give_copy(i):
        return pltpu.make_async_remote_copy(
            src_ref=give_ref.at[i], dst_ref=take_ref.at[i], send_sem=give_send.at[i], recv_sem=take_recv.at[i],
            device_id=to_twin, device_id_type=MESH,
        )

    def give(i, _):
        give_ref[i] = product((1 - core) * pairs + i).astype(jnp.bfloat16)

        @pl.when(i > 0)
        def _():
            give_copy(i - 1).start()

        return 0

    lax.fori_loop(0, pairs, give, 0)
    give_copy(pairs - 1).start()

    def keep(i, _):
        total = product(core * pairs + i)
        give_copy(i).wait_recv()
        columns = pl.ds(pl.multiple_of(i * give_ref.shape[2], give_ref.shape[2]), give_ref.shape[2])
        out_ref[:, columns] = (total + take_ref[i].astype(jnp.float32)).astype(jnp.bfloat16)
        return 0

    lax.fori_loop(0, pairs, keep, 0)

    def sent(s, _):
        a, b = behind(s), ahead(s)
        k_copy(0, a).wait_send()
        v_copy(1, b).wait_send()

        @pl.when(s < steps - 1)
        def _():
            k_copy(1, b).wait_send()
            v_copy(0, a).wait_send()
            w_copy(0, a).wait_send()
            w_copy(1, b).wait_send()

        @pl.when(s == steps - 1)
        def _():
            w_last_copy(0, a).wait_send()
            w_last_copy(1, b).wait_send()

        return 0

    lax.fori_loop(1, steps, sent, 0)
    for d in (0, 1):
        for copy in (k_copy, v_copy, w_copy):
            copy(d, me).wait_send()

    def passed(s, _):
        slot = ahead(s)
        x_copy(slot, mine).wait_send()
        y_copy(slot, mine).wait_send()
        yd_copy(slot, of_x).wait_send()
        xd_copy(slot, of_y).wait_send()
        return 0

    lax.fori_loop(1, n, passed, 0)

    def given(i, _):
        give_copy(i).wait_send()
        return 0

    lax.fori_loop(0, pairs, given, 0)


def local(n, row_stride, query_states, key_states, value_rows, positions, out_weight):
    tokens, query_heads, head_size = query_states.shape
    kv_heads = key_states.shape[1]
    heads = query_heads // kv_heads
    half = tokens // 2
    rows, slab = out_weight.shape
    pairs = n // 4
    width = heads * half
    grouped = query_states.reshape(2, half, kv_heads, heads, head_size).transpose(2, 0, 4, 3, 1)
    grouped = grouped.reshape(kv_heads, 2, head_size, width)
    place = (positions[0] // half).astype(jnp.bfloat16)
    tagged = jnp.concatenate(
        [
            key_states.transpose(1, 0, 2).reshape(kv_heads * tokens, head_size),
            jnp.broadcast_to(place, (TAG_ROWS, head_size)),
        ],
        axis=0,
    )
    turned = value_rows.transpose(1, 2, 0)
    dma, bf16, f32 = pltpu.SemaphoreType.DMA, jnp.bfloat16, jnp.float32
    anywhere = pl.BlockSpec(memory_space=pl.ANY)
    return pl.pallas_call(
        functools.partial(kernel, n, row_stride, kv_heads, half),
        out_shape=jax.ShapeDtypeStruct((tokens, n // 2 * slab), bf16),
        in_specs=[anywhere] * 4,
        out_specs=pl.BlockSpec(memory_space=pltpu.VMEM),
        scratch_shapes=[
            pltpu.VMEM(grouped.shape, bf16),
            pltpu.VMEM((n,) + tagged.shape, bf16),
            pltpu.VMEM((n,) + turned.shape, bf16),
            pltpu.VMEM((n, rows, slab), bf16),
            pltpu.VMEM((kv_heads, 2, head_size, width), f32),
            pltpu.VMEM((kv_heads, 2, 1, width), f32),
            pltpu.VMEM((kv_heads, 2, 1, width), f32),
            pltpu.VMEM((tokens, query_heads * head_size), bf16),
            pltpu.VMEM((pairs, tokens, 2 * slab), bf16),
            pltpu.VMEM((pairs, tokens, 2 * slab), bf16),
            dma((4,)),
            dma((2, n)),
            dma((2, n)),
            dma((2, n)),
            dma((n,)),
            dma((n,)),
            dma((n,)),
            dma((n,)),
            dma((n,)),
            dma((n,)),
            dma((n,)),
            dma((1,)),
            dma((n,)),
            dma((n,)),
            dma((n,)),
            dma((n,)),
            dma((pairs,)),
            dma((pairs,)),
        ],
        compiler_params=pltpu.CompilerParams(
            collective_id=0, has_side_effects=True, vmem_limit_bytes=62 * 1024 * 1024
        ),
    )(grouped, tagged, turned, out_weight)


def solution(mesh):
    n, groups = mesh.shape["ctx"], mesh.shape["groups"]
    row_stride = 1 << ((groups.bit_length() - 1) // 2)
    assert n % 4 == 0 and row_stride % 2 == 0 and groups % (2 * row_stride) == 0
    in_specs = (
        P(("groups", "ctx"), "tp", None),
        P(("groups", "ctx"), "tp", None),
        P(("groups", "ctx"), "tp", None),
        P(("groups", "ctx")),
        P("tp", "ctx"),
    )
    out_specs = P(("groups", "ctx"), "tp")
    return jax.shard_map(
        functools.partial(local, n, row_stride),
        mesh=mesh, in_specs=in_specs, out_specs=out_specs, check_vma=False,
    )
```

```python
import functools

import jax
import jax.numpy as jnp
from jax import lax
from jax.experimental import pallas as pl
from jax.experimental.pallas import tpu as pltpu
from jax.sharding import PartitionSpec as P

MESH = pl.DeviceIdType.MESH
LOG2E = 1.4426950408889634
LOW = -1e30
HIGH = 1e30
TAG_ROWS = 16
LANES = 1024


def flip(index, stride):
    return index + stride * (1 - 2 * lax.rem(index // stride, 2))


def kernel(
    n, row_stride, kv_heads, half, q_hbm, k_hbm, v_hbm, p_hbm, w_hbm, out_ref,
    q_raw, k_raw, v_raw, p_raw, q_ref, kbuf, vbuf, wbuf, acc_ref, max_ref, sum_ref, att_ref, give_ref, take_ref,
    in_sem, k_send, v_send, w_send, x_send, y_send, xd_send, yd_send,
    k_recv, v_recv, w_recv, w_last_recv, x_recv, y_recv, xd_recv, yd_recv, give_send, take_recv,
):
    me, group, core = (lax.axis_index(a) for a in ("ctx", "groups", "tp"))
    head_size = q_ref.shape[2]
    width = q_ref.shape[3]
    chunks = width // LANES
    keys = 2 * half
    scale = LOG2E * head_size ** (-0.5)
    rows = wbuf.shape[1]
    quarter, eighth = rows // 4, rows // 8
    steps = n // 2

    right, left = lax.rem(me + 1, n), lax.rem(me + n - 1, n)
    x_group, y_group = flip(group, 1), flip(group, row_stride)
    px, py = lax.rem(group, 2), lax.rem(group // row_stride, 2)
    mine = pl.multiple_of((2 * py + px) * quarter, quarter)
    of_x = pl.multiple_of((2 * py + 1 - px) * quarter, quarter)
    of_y = pl.multiple_of((2 * (1 - py) + px) * quarter, quarter)
    of_xy = pl.multiple_of((2 * (1 - py) + 1 - px) * quarter, quarter)
    to_right, to_left = {"ctx": right}, {"ctx": left}
    to_x, to_y, to_twin = {"groups": x_group}, {"groups": y_group}, {"tp": 1 - core}

    def remote(ref, send, recv, device):
        return pltpu.make_async_remote_copy(
            src_ref=ref, dst_ref=ref, send_sem=send, recv_sem=recv, device_id=device, device_id_type=MESH
        )

    def way(d):
        return to_right if d == 0 else to_left

    def k_copy(d, slot):
        return remote(kbuf.at[slot], k_send.at[d, slot], k_recv.at[slot], way(d))

    def v_copy(d, slot):
        return remote(vbuf.at[slot], v_send.at[d, slot], v_recv.at[slot], way(d))

    def w_copy(d, slot):
        return remote(wbuf.at[slot, pl.ds(mine, quarter)], w_send.at[d, slot], w_recv.at[slot], way(d))

    def w_last_copy(d, slot):
        ref = wbuf.at[slot, pl.ds(mine + d * eighth, eighth)]
        return remote(ref, w_send.at[d, slot], w_recv.at[slot] if d == 0 else w_last_recv.at[0], way(d))

    def x_copy(slot, start):
        return remote(wbuf.at[slot, pl.ds(start, quarter)], x_send.at[slot], x_recv.at[slot], to_x)

    def y_copy(slot, start):
        return remote(wbuf.at[slot, pl.ds(start, quarter)], y_send.at[slot], y_recv.at[slot], to_y)

    def xd_copy(slot, start):
        return remote(wbuf.at[slot, pl.ds(start, eighth)], xd_send.at[slot], xd_recv.at[slot], to_x)

    def yd_copy(slot, start):
        return remote(wbuf.at[slot, pl.ds(start + eighth, eighth)], yd_send.at[slot], yd_recv.at[slot], to_y)

    def side(slot):
        x_copy(slot, mine).start()
        y_copy(slot, mine).start()

    def relay(slot):
        x_copy(slot, of_x).wait_recv()
        yd_copy(slot, of_x).start()
        y_copy(slot, of_y).wait_recv()
        xd_copy(slot, of_y).start()

    own = (
        pltpu.make_async_copy(w_hbm, wbuf.at[me], in_sem.at[0]),
        pltpu.make_async_copy(k_hbm, k_raw, in_sem.at[1]),
        pltpu.make_async_copy(p_hbm, p_raw, in_sem.at[2]),
        pltpu.make_async_copy(v_hbm, v_raw, in_sem.at[3]),
        pltpu.make_async_copy(q_hbm, q_raw, in_sem.at[4]),
    )
    for copy in own:
        copy.start()

    barrier = pltpu.get_barrier_semaphore()
    for device in (to_right, to_left, to_x, to_y, to_twin):
        pl.semaphore_signal(barrier, inc=1, device_id=device, device_id_type=MESH)
    pl.semaphore_wait(barrier, 5)

    own[0].wait()
    for d in (0, 1):
        w_copy(d, me).start()

    own[1].wait()
    own[2].wait()
    for kv in range(kv_heads):
        kbuf[me, kv * keys : (kv + 1) * keys, :] = k_raw[:, kv, :]
    place = p_raw[0:1, 0:1].astype(jnp.float32) / half
    kbuf[me, kv_heads * keys :, :] = jnp.broadcast_to(place, (TAG_ROWS, head_size)).astype(jnp.bfloat16)
    own[3].wait()
    for kv in range(kv_heads):
        vbuf[me, kv] = v_raw[:, kv, :].T
    for d in (0, 1):
        k_copy(d, me).start()

    own[4].wait()
    heads = width // half
    for kv in range(kv_heads):
        for h in range(heads):
            turned = q_raw[:, kv * heads + h, :].T
            for part in (0, 1):
                q_ref[kv, part, :, h * half : (h + 1) * half] = turned[:, part * half : (part + 1) * half]
        if kv == 0:
            for d in (0, 1):
                v_copy(d, me).start()

    def places(i):
        kv = i // chunks
        return kv, pl.ds(pl.multiple_of(lax.rem(i, chunks) * LANES, LANES), LANES)

    def scores_of(key_part, kv, part, lanes):
        return jnp.dot(key_part, q_ref[kv, part, :, lanes], preferred_element_type=jnp.float32)

    def powers(scores, shift):
        return jnp.exp2((scores - shift) * scale)

    def column_max(scores):
        return jnp.max(scores, axis=0, keepdims=True)

    def column_sum(values):
        return jnp.sum(values, axis=0, keepdims=True)

    def first(i, _):
        kv, lanes = places(i)
        key_rows = pl.multiple_of(kv * keys, keys)
        key_block = kbuf[me, pl.ds(key_rows, keys), :]
        values = vbuf[me, kv]
        shape = (half, LANES)
        tri = lax.broadcasted_iota(jnp.int32, shape, 0) <= lax.rem(lax.broadcasted_iota(jnp.int32, shape, 1), half)
        for part in (0, 1):
            scores = scores_of(key_block[: half * (part + 1)], kv, part, lanes)
            pieces = [scores[half * j : half * (j + 1)] for j in range(part + 1)]
            pieces[part] = jnp.where(tri, pieces[part], LOW)
            largest = functools.reduce(jnp.maximum, [column_max(p) for p in pieces])
            exps = jnp.concatenate([powers(p, largest) for p in pieces], axis=0)
            max_ref[kv, part, :, lanes] = largest
            sum_ref[kv, part, :, lanes] = column_sum(exps)
            acc_ref[kv, part, :, lanes] = jnp.dot(
                values[:, : half * (part + 1)], exps.astype(jnp.bfloat16), preferred_element_type=jnp.float32
            )
        return 0

    lax.fori_loop(0, kv_heads * chunks, first, 0)

    def tag(slot):
        row = kbuf[slot, kv_heads * keys :, :].astype(jnp.float32)[:1]
        return jnp.concatenate([row] * (LANES // row.shape[1]), axis=1)

    def attend(slot):
        theirs, ours = tag(slot), tag(me)
        before, after = theirs < ours, theirs > ours

        def one(i, _):
            kv, lanes = places(i)
            key_rows = pl.multiple_of(kv * keys, keys)
            key_block = kbuf[slot, pl.ds(key_rows, keys), :]
            values = vbuf[slot, kv]

            def renew(part, largest, shifts, pieces, value_part):
                old = max_ref[kv, part, :, lanes]
                factor = jnp.exp2((old - largest) * scale)
                exps = jnp.concatenate([powers(p, s) for p, s in zip(pieces, shifts)], axis=0)
                max_ref[kv, part, :, lanes] = largest
                sum_ref[kv, part, :, lanes] = sum_ref[kv, part, :, lanes] * factor + column_sum(exps)
                acc_ref[kv, part, :, lanes] = acc_ref[kv, part, :, lanes] * factor + jnp.dot(
                    value_part, exps.astype(jnp.bfloat16), preferred_element_type=jnp.float32
                )

            low = scores_of(key_block[:half], kv, 0, lanes)
            largest = jnp.maximum(max_ref[kv, 0, :, lanes], jnp.where(before, column_max(low), LOW))
            renew(0, largest, [jnp.where(before, largest, HIGH)], [low], values[:, :half])

            high = scores_of(key_block, kv, 1, lanes)
            pieces = [high[:half], high[half:]]
            largest = jnp.maximum(column_max(pieces[0]), jnp.where(after, column_max(pieces[1]), LOW))
            largest = jnp.maximum(max_ref[kv, 1, :, lanes], largest)
            renew(1, largest, [largest, jnp.where(after, largest, HIGH)], pieces, values)
            return 0

        lax.fori_loop(0, kv_heads * chunks, one, 0)

    def behind(s):
        return lax.rem(me + n - s, n)

    def ahead(s):
        return lax.rem(me + s, n)

    def step(s, _):
        a, b = behind(s), ahead(s)
        w_copy(0, a).wait_recv()
        w_copy(1, b).wait_recv()

        @pl.when(s < steps - 1)
        def _():
            w_copy(0, a).start()
            w_copy(1, b).start()

        @pl.when(s == steps - 1)
        def _():
            w_last_copy(0, a).start()
            w_last_copy(1, b).start()

        side(a)
        side(b)

        @pl.when(s > 1)
        def _():
            attend(ahead(s - 1))

        k_copy(0, a).wait_recv()
        k_copy(0, a).start()
        k_copy(1, b).wait_recv()

        @pl.when(s < steps - 1)
        def _():
            k_copy(1, b).start()

        v_copy(0, a).wait_recv()

        @pl.when(s < steps - 1)
        def _():
            v_copy(0, a).start()

        v_copy(1, b).wait_recv()
        v_copy(1, b).start()

        @pl.when(s > 1)
        def _():
            relay(behind(s - 1))
            relay(ahead(s - 1))

        attend(a)
        return 0

    lax.fori_loop(1, steps, step, 0)

    far = ahead(steps)
    w_last_copy(0, far).wait_recv()
    w_last_copy(1, far).wait_recv()
    side(far)
    attend(ahead(steps - 1))
    relay(behind(steps - 1))
    relay(ahead(steps - 1))
    k_copy(0, far).wait_recv()
    v_copy(1, far).wait_recv()
    attend(far)
    relay(far)

    def finish(i, _):
        kv, part = i // 2, lax.rem(i, 2)
        for h in range(heads):
            lanes = slice(h * half, (h + 1) * half)
            tile = acc_ref[kv, part, :, lanes] * (1.0 / sum_ref[kv, part, :, lanes])
            columns = pl.ds(pl.multiple_of((kv * heads + h) * head_size, head_size), head_size)
            att_ref[pl.ds(pl.multiple_of(part * half, half), half), columns] = tile.T.astype(jnp.bfloat16)
        return 0

    lax.fori_loop(0, kv_heads * 2, finish, 0)

    def arrived(s, _):
        slot = ahead(s)
        xd_copy(slot, of_xy).wait_recv()
        yd_copy(slot, of_xy).wait_recv()
        return 0

    lax.fori_loop(1, n, arrived, 0)

    pairs = n // 4

    def product(pair):
        weight = jnp.concatenate([wbuf[2 * pair], wbuf[2 * pair + 1]], axis=1)
        return jnp.dot(att_ref[...], weight, preferred_element_type=jnp.float32)

    def give_copy(i):
        return pltpu.make_async_remote_copy(
            src_ref=give_ref.at[i], dst_ref=take_ref.at[i], send_sem=give_send.at[i], recv_sem=take_recv.at[i],
            device_id=to_twin, device_id_type=MESH,
        )

    def give(i, _):
        give_ref[i] = product((1 - core) * pairs + i).astype(jnp.bfloat16)

        @pl.when(i > 0)
        def _():
            give_copy(i - 1).start()

        return 0

    lax.fori_loop(0, pairs, give, 0)
    give_copy(pairs - 1).start()

    def keep(i, _):
        total = product(core * pairs + i)
        give_copy(i).wait_recv()
        columns = pl.ds(pl.multiple_of(i * give_ref.shape[2], give_ref.shape[2]), give_ref.shape[2])
        out_ref[:, columns] = (total + take_ref[i].astype(jnp.float32)).astype(jnp.bfloat16)
        return 0

    lax.fori_loop(0, pairs, keep, 0)

    def sent(s, _):
        a, b = behind(s), ahead(s)
        k_copy(0, a).wait_send()
        v_copy(1, b).wait_send()

        @pl.when(s < steps - 1)
        def _():
            k_copy(1, b).wait_send()
            v_copy(0, a).wait_send()
            w_copy(0, a).wait_send()
            w_copy(1, b).wait_send()

        @pl.when(s == steps - 1)
        def _():
            w_last_copy(0, a).wait_send()
            w_last_copy(1, b).wait_send()

        return 0

    lax.fori_loop(1, steps, sent, 0)
    for d in (0, 1):
        for copy in (k_copy, v_copy, w_copy):
            copy(d, me).wait_send()

    def passed(s, _):
        slot = ahead(s)
        x_copy(slot, mine).wait_send()
        y_copy(slot, mine).wait_send()
        yd_copy(slot, of_x).wait_send()
        xd_copy(slot, of_y).wait_send()
        return 0

    lax.fori_loop(1, n, passed, 0)

    def given(i, _):
        give_copy(i).wait_send()
        return 0

    lax.fori_loop(0, pairs, given, 0)


def local(n, row_stride, query_states, key_states, value_rows, positions, out_weight):
    tokens, query_heads, head_size = query_states.shape
    kv_heads = key_states.shape[1]
    heads = query_heads // kv_heads
    half = tokens // 2
    rows, slab = out_weight.shape
    pairs = n // 4
    width = heads * half
    dma, bf16, f32 = pltpu.SemaphoreType.DMA, jnp.bfloat16, jnp.float32
    anywhere = pl.BlockSpec(memory_space=pl.ANY)
    return pl.pallas_call(
        functools.partial(kernel, n, row_stride, kv_heads, half),
        out_shape=jax.ShapeDtypeStruct((tokens, n // 2 * slab), bf16),
        in_specs=[anywhere] * 5,
        out_specs=pl.BlockSpec(memory_space=pltpu.VMEM),
        scratch_shapes=[
            pltpu.VMEM(query_states.shape, bf16),
            pltpu.VMEM(key_states.shape, bf16),
            pltpu.VMEM(value_rows.shape, bf16),
            pltpu.VMEM((2, half), positions.dtype),
            pltpu.VMEM((kv_heads, 2, head_size, width), bf16),
            pltpu.VMEM((n, kv_heads * tokens + TAG_ROWS, head_size), bf16),
            pltpu.VMEM((n, kv_heads, head_size, tokens), bf16),
            pltpu.VMEM((n, rows, slab), bf16),
            pltpu.VMEM((kv_heads, 2, head_size, width), f32),
            pltpu.VMEM((kv_heads, 2, 1, width), f32),
            pltpu.VMEM((kv_heads, 2, 1, width), f32),
            pltpu.VMEM((tokens, query_heads * head_size), bf16),
            pltpu.VMEM((pairs, tokens, 2 * slab), bf16),
            pltpu.VMEM((pairs, tokens, 2 * slab), bf16),
            dma((5,)),
            dma((2, n)),
            dma((2, n)),
            dma((2, n)),
            dma((n,)),
            dma((n,)),
            dma((n,)),
            dma((n,)),
            dma((n,)),
            dma((n,)),
            dma((n,)),
            dma((1,)),
            dma((n,)),
            dma((n,)),
            dma((n,)),
            dma((n,)),
            dma((pairs,)),
            dma((pairs,)),
        ],
        compiler_params=pltpu.CompilerParams(
            collective_id=0, has_side_effects=True, vmem_limit_bytes=62 * 1024 * 1024
        ),
    )(query_states, key_states, value_rows, positions.reshape(2, half), out_weight)


def solution(mesh):
    n, groups = mesh.shape["ctx"], mesh.shape["groups"]
    row_stride = 1 << ((groups.bit_length() - 1) // 2)
    assert n % 4 == 0 and row_stride % 2 == 0 and groups % (2 * row_stride) == 0
    in_specs = (
        P(("groups", "ctx"), "tp", None),
        P(("groups", "ctx"), "tp", None),
        P(("groups", "ctx"), "tp", None),
        P(("groups", "ctx")),
        P("tp", "ctx"),
    )
    out_specs = P(("groups", "ctx"), "tp")
    return jax.shard_map(
        functools.partial(local, n, row_stride),
        mesh=mesh, in_specs=in_specs, out_specs=out_specs, check_vma=False,
    )
```

```python
import functools

import jax
import jax.numpy as jnp
from jax import lax
from jax.experimental import pallas as pl
from jax.experimental.pallas import tpu as pltpu
from jax.sharding import PartitionSpec as P

MESH = pl.DeviceIdType.MESH
LOG2E = 1.4426950408889634
LOW = -1e30
HIGH = 1e30
TAG_ROWS = 16
LANES = 1024
SLABS = 4


def flip(index, stride):
    return index + stride * (1 - 2 * lax.rem(index // stride, 2))


def kernel(
    n, row_stride, kv_heads, half, q_hbm, k_hbm, v_hbm, p_hbm, w_hbm, out_hbm,
    q_raw, k_raw, v_raw, p_raw, q_ref, kbuf, vbuf, wbuf, acc_ref, max_ref, sum_ref, att_ref, give_ref, take_ref, total_ref,
    in_sem, k_send, v_send, w_send, x_send, y_send, xd_send, yd_send,
    k_recv, v_recv, w_recv, w_last_recv, x_recv, y_recv, xd_recv, yd_recv, give_send, take_recv, out_sem,
):
    me, group, core = (lax.axis_index(a) for a in ("ctx", "groups", "tp"))
    head_size = q_ref.shape[2]
    width = q_ref.shape[3]
    chunks = width // LANES
    keys = 2 * half
    scale = LOG2E * head_size ** (-0.5)
    rows = wbuf.shape[1]
    quarter, eighth = rows // 4, rows // 8
    steps = n // 2

    right, left = lax.rem(me + 1, n), lax.rem(me + n - 1, n)
    x_group, y_group = flip(group, 1), flip(group, row_stride)
    px, py = lax.rem(group, 2), lax.rem(group // row_stride, 2)
    mine = pl.multiple_of((2 * py + px) * quarter, quarter)
    of_x = pl.multiple_of((2 * py + 1 - px) * quarter, quarter)
    of_y = pl.multiple_of((2 * (1 - py) + px) * quarter, quarter)
    of_xy = pl.multiple_of((2 * (1 - py) + 1 - px) * quarter, quarter)
    to_right, to_left = {"ctx": right}, {"ctx": left}
    to_x, to_y, to_twin = {"groups": x_group}, {"groups": y_group}, {"tp": 1 - core}

    def remote(ref, send, recv, device):
        return pltpu.make_async_remote_copy(
            src_ref=ref, dst_ref=ref, send_sem=send, recv_sem=recv, device_id=device, device_id_type=MESH
        )

    def way(d):
        return to_right if d == 0 else to_left

    def k_copy(d, slot):
        return remote(kbuf.at[slot], k_send.at[d, slot], k_recv.at[slot], way(d))

    def v_copy(d, slot):
        return remote(vbuf.at[slot], v_send.at[d, slot], v_recv.at[slot], way(d))

    def w_copy(d, slot):
        return remote(wbuf.at[slot, pl.ds(mine, quarter)], w_send.at[d, slot], w_recv.at[slot], way(d))

    def w_last_copy(d, slot):
        ref = wbuf.at[slot, pl.ds(mine + d * eighth, eighth)]
        return remote(ref, w_send.at[d, slot], w_recv.at[slot] if d == 0 else w_last_recv.at[0], way(d))

    def x_copy(slot, start):
        return remote(wbuf.at[slot, pl.ds(start, quarter)], x_send.at[slot], x_recv.at[slot], to_x)

    def y_copy(slot, start):
        return remote(wbuf.at[slot, pl.ds(start, quarter)], y_send.at[slot], y_recv.at[slot], to_y)

    def xd_copy(slot, start):
        return remote(wbuf.at[slot, pl.ds(start, eighth)], xd_send.at[slot], xd_recv.at[slot], to_x)

    def yd_copy(slot, start):
        return remote(wbuf.at[slot, pl.ds(start + eighth, eighth)], yd_send.at[slot], yd_recv.at[slot], to_y)

    def side(slot):
        x_copy(slot, mine).start()
        y_copy(slot, mine).start()

    def relay(slot):
        x_copy(slot, of_x).wait_recv()
        yd_copy(slot, of_x).start()
        y_copy(slot, of_y).wait_recv()
        xd_copy(slot, of_y).start()

    own = (
        pltpu.make_async_copy(w_hbm, wbuf.at[me], in_sem.at[0]),
        pltpu.make_async_copy(k_hbm, k_raw, in_sem.at[1]),
        pltpu.make_async_copy(p_hbm, p_raw, in_sem.at[2]),
        pltpu.make_async_copy(v_hbm, v_raw, in_sem.at[3]),
        pltpu.make_async_copy(q_hbm, q_raw, in_sem.at[4]),
    )
    for copy in own:
        copy.start()

    barrier = pltpu.get_barrier_semaphore()
    for device in (to_right, to_left, to_x, to_y, to_twin):
        pl.semaphore_signal(barrier, inc=1, device_id=device, device_id_type=MESH)
    pl.semaphore_wait(barrier, 5)

    own[0].wait()
    for d in (0, 1):
        w_copy(d, me).start()

    own[1].wait()
    own[2].wait()
    for kv in range(kv_heads):
        kbuf[me, kv * keys : (kv + 1) * keys, :] = k_raw[:, kv, :]
    place = p_raw[0:1, 0:1].astype(jnp.float32) / half
    kbuf[me, kv_heads * keys :, :] = jnp.broadcast_to(place, (TAG_ROWS, head_size)).astype(jnp.bfloat16)
    own[3].wait()
    for kv in range(kv_heads):
        vbuf[me, kv] = v_raw[:, kv, :].T
    for d in (0, 1):
        k_copy(d, me).start()

    own[4].wait()
    heads = width // half
    for kv in range(kv_heads):
        for h in range(heads):
            turned = q_raw[:, kv * heads + h, :].T
            for part in (0, 1):
                q_ref[kv, part, :, h * half : (h + 1) * half] = turned[:, part * half : (part + 1) * half]
        if kv == 0:
            for d in (0, 1):
                v_copy(d, me).start()

    def places(i):
        kv = i // chunks
        return kv, pl.ds(pl.multiple_of(lax.rem(i, chunks) * LANES, LANES), LANES)

    def scores_of(key_part, kv, part, lanes):
        return jnp.dot(key_part, q_ref[kv, part, :, lanes], preferred_element_type=jnp.float32)

    def powers(scores, shift):
        return jnp.exp2((scores - shift) * scale)

    def column_max(scores):
        return jnp.max(scores, axis=0, keepdims=True)

    def column_sum(values):
        return jnp.sum(values, axis=0, keepdims=True)

    def first(i, _):
        kv, lanes = places(i)
        key_rows = pl.multiple_of(kv * keys, keys)
        key_block = kbuf[me, pl.ds(key_rows, keys), :]
        values = vbuf[me, kv]
        shape = (half, LANES)
        tri = lax.broadcasted_iota(jnp.int32, shape, 0) <= lax.rem(lax.broadcasted_iota(jnp.int32, shape, 1), half)
        for part in (0, 1):
            scores = scores_of(key_block[: half * (part + 1)], kv, part, lanes)
            pieces = [scores[half * j : half * (j + 1)] for j in range(part + 1)]
            pieces[part] = jnp.where(tri, pieces[part], LOW)
            largest = functools.reduce(jnp.maximum, [column_max(p) for p in pieces])
            exps = jnp.concatenate([powers(p, largest) for p in pieces], axis=0)
            max_ref[kv, part, :, lanes] = largest
            sum_ref[kv, part, :, lanes] = column_sum(exps)
            acc_ref[kv, part, :, lanes] = jnp.dot(
                values[:, : half * (part + 1)], exps.astype(jnp.bfloat16), preferred_element_type=jnp.float32
            )
        return 0

    lax.fori_loop(0, kv_heads * chunks, first, 0)

    def tag(slot):
        row = kbuf[slot, kv_heads * keys :, :].astype(jnp.float32)[:1]
        return jnp.concatenate([row] * (LANES // row.shape[1]), axis=1)

    def attend(slot, kv):
        theirs, ours = tag(slot), tag(me)
        before, after = theirs < ours, theirs > ours

        def one(i, _):
            lanes = pl.ds(pl.multiple_of(i * LANES, LANES), LANES)
            key_rows = pl.multiple_of(kv * keys, keys)
            key_block = kbuf[slot, pl.ds(key_rows, keys), :]
            values = vbuf[slot, kv]

            def renew(part, largest, shifts, pieces, value_part):
                old = max_ref[kv, part, :, lanes]
                factor = jnp.exp2((old - largest) * scale)
                exps = jnp.concatenate([powers(p, s) for p, s in zip(pieces, shifts)], axis=0)
                max_ref[kv, part, :, lanes] = largest
                sum_ref[kv, part, :, lanes] = sum_ref[kv, part, :, lanes] * factor + column_sum(exps)
                acc_ref[kv, part, :, lanes] = acc_ref[kv, part, :, lanes] * factor + jnp.dot(
                    value_part, exps.astype(jnp.bfloat16), preferred_element_type=jnp.float32
                )

            low = scores_of(key_block[:half], kv, 0, lanes)
            largest = jnp.maximum(max_ref[kv, 0, :, lanes], jnp.where(before, column_max(low), LOW))
            renew(0, largest, [jnp.where(before, largest, HIGH)], [low], values[:, :half])

            high = scores_of(key_block, kv, 1, lanes)
            pieces = [high[:half], high[half:]]
            largest = jnp.maximum(column_max(pieces[0]), jnp.where(after, column_max(pieces[1]), LOW))
            largest = jnp.maximum(max_ref[kv, 1, :, lanes], largest)
            renew(1, largest, [largest, jnp.where(after, largest, HIGH)], pieces, values)
            return 0

        lax.fori_loop(0, chunks, one, 0)

    def attend_all(slot):
        def one(kv, _):
            attend(slot, kv)
            return 0

        lax.fori_loop(0, kv_heads, one, 0)

    def behind(s):
        return lax.rem(me + n - s, n)

    def ahead(s):
        return lax.rem(me + s, n)

    def arrived_at(slot):
        xd_copy(slot, of_xy).wait_recv()
        yd_copy(slot, of_xy).wait_recv()

    def arrived(s):
        arrived_at(behind(s))
        arrived_at(ahead(s))

    def sent_aside(slot):
        x_copy(slot, mine).wait_send()
        y_copy(slot, mine).wait_send()
        yd_copy(slot, of_x).wait_send()
        xd_copy(slot, of_y).wait_send()

    def sent(s):
        a, b = behind(s), ahead(s)
        k_copy(0, a).wait_send()
        v_copy(1, b).wait_send()

        @pl.when(s < steps - 1)
        def _():
            k_copy(1, b).wait_send()
            v_copy(0, a).wait_send()
            w_copy(0, a).wait_send()
            w_copy(1, b).wait_send()

        @pl.when(s == steps - 1)
        def _():
            w_last_copy(0, a).wait_send()
            w_last_copy(1, b).wait_send()

        sent_aside(a)
        sent_aside(b)

    def each(low, high, what):
        def one(s, _):
            what(s)
            return 0

        lax.fori_loop(max(low, 1), high, one, 0)

    def step(s, _):
        a, b = behind(s), ahead(s)
        w_copy(0, a).wait_recv()
        w_copy(1, b).wait_recv()

        @pl.when(s < steps - 1)
        def _():
            w_copy(0, a).start()
            w_copy(1, b).start()

        @pl.when(s == steps - 1)
        def _():
            w_last_copy(0, a).start()
            w_last_copy(1, b).start()

        side(a)
        side(b)

        @pl.when(s > 1)
        def _():
            relay(behind(s - 1))
            relay(ahead(s - 1))

        @pl.when(s > 1)
        def _():
            attend(ahead(s - 1), 0)

        k_copy(0, a).wait_recv()
        k_copy(0, a).start()
        k_copy(1, b).wait_recv()

        @pl.when(s < steps - 1)
        def _():
            k_copy(1, b).start()

        @pl.when(s > 1)
        def _():
            attend(ahead(s - 1), 1)

        v_copy(0, a).wait_recv()

        @pl.when(s < steps - 1)
        def _():
            v_copy(0, a).start()

        v_copy(1, b).wait_recv()
        v_copy(1, b).start()

        @pl.when(s > 2)
        def _():
            arrived(s - 2)

        @pl.when(s > 3)
        def _():
            sent(s - 3)

        attend_all(a)
        return 0

    lax.fori_loop(1, steps, step, 0)

    far = ahead(steps)
    w_last_copy(0, far).wait_recv()
    w_last_copy(1, far).wait_recv()
    side(far)
    relay(behind(steps - 1))
    relay(ahead(steps - 1))
    attend_all(ahead(steps - 1))
    k_copy(0, far).wait_recv()
    v_copy(1, far).wait_recv()
    attend_all(far)

    def finish(i, _):
        kv, part = i // 2, lax.rem(i, 2)
        for h in range(heads):
            lanes = slice(h * half, (h + 1) * half)
            tile = acc_ref[kv, part, :, lanes] * (1.0 / sum_ref[kv, part, :, lanes])
            columns = pl.ds(pl.multiple_of((kv * heads + h) * head_size, head_size), head_size)
            att_ref[pl.ds(pl.multiple_of(part * half, half), half), columns] = tile.T.astype(jnp.bfloat16)
        return 0

    lax.fori_loop(0, kv_heads * 2, finish, 0)

    relay(far)
    each(steps - 2, steps, arrived)

    parts = give_ref.shape[0]
    slabs = n // (2 * parts)
    span = give_ref.shape[2]
    far_part = lax.rem(far // slabs, parts)
    far_given = lax.rem(far // (slabs * parts) + core, 2)

    def turn(i):
        late = jnp.where(i < parts - 1, i, jnp.where(i < 2 * parts - 1, i + 1, parts - 1))
        turn = jnp.where(far_given == 1, late, i)
        return turn < parts, lax.rem(far_part + 1 + lax.rem(turn, parts), parts)

    def give_copy(part):
        return pltpu.make_async_remote_copy(
            src_ref=give_ref.at[part], dst_ref=take_ref.at[part], send_sem=give_send.at[part],
            recv_sem=take_recv.at[part], device_id=to_twin, device_id_type=MESH,
        )

    def out_copy(part):
        columns = pl.ds(pl.multiple_of(part * span, span), span)
        return pltpu.make_async_copy(total_ref.at[part], out_hbm.at[:, columns], out_sem.at[part])

    def pass_on(i):
        given, part = turn(i)

        @pl.when(given)
        def _():
            give_copy(part).start()

        @pl.when(jnp.logical_not(given))
        def _():
            out_copy(part).start()

    def project(i, _):
        given, part = turn(i)
        first_slab = slabs * (part + parts * jnp.where(given, 1 - core, core))

        @pl.when(i == 2 * parts - 1)
        def _():
            arrived_at(far)

        weight = jnp.concatenate([wbuf[first_slab + j] for j in range(slabs)], axis=1)
        product = jnp.dot(att_ref[...], weight, preferred_element_type=jnp.float32)

        @pl.when(i > 0)
        def _():
            pass_on(i - 1)

        @pl.when(given)
        def _():
            give_ref[part] = product.astype(jnp.bfloat16)

        @pl.when(jnp.logical_not(given))
        def _():
            give_copy(part).wait_recv()
            total_ref[part] = (product + take_ref[part].astype(jnp.float32)).astype(jnp.bfloat16)

        return 0

    lax.fori_loop(0, 2 * parts, project, 0)
    pass_on(2 * parts - 1)

    each(steps - 3, steps, sent)
    sent_aside(far)
    for d in (0, 1):
        for copy in (k_copy, v_copy, w_copy):
            copy(d, me).wait_send()
    for part in range(parts):
        give_copy(part).wait_send()
        out_copy(part).wait()


def local(n, row_stride, query_states, key_states, value_rows, positions, out_weight):
    tokens, query_heads, head_size = query_states.shape
    kv_heads = key_states.shape[1]
    heads = query_heads // kv_heads
    half = tokens // 2
    rows, slab = out_weight.shape
    parts = max(n // (2 * SLABS), 1)
    slabs = n // (2 * parts)
    width = heads * half
    dma, bf16, f32 = pltpu.SemaphoreType.DMA, jnp.bfloat16, jnp.float32
    anywhere = pl.BlockSpec(memory_space=pl.ANY)
    return pl.pallas_call(
        functools.partial(kernel, n, row_stride, kv_heads, half),
        out_shape=jax.ShapeDtypeStruct((tokens, n // 2 * slab), bf16),
        in_specs=[anywhere] * 5,
        out_specs=anywhere,
        scratch_shapes=[
            pltpu.VMEM(query_states.shape, bf16),
            pltpu.VMEM(key_states.shape, bf16),
            pltpu.VMEM(value_rows.shape, bf16),
            pltpu.VMEM((2, half), positions.dtype),
            pltpu.VMEM((kv_heads, 2, head_size, width), bf16),
            pltpu.VMEM((n, kv_heads * tokens + TAG_ROWS, head_size), bf16),
            pltpu.VMEM((n, kv_heads, head_size, tokens), bf16),
            pltpu.VMEM((n, rows, slab), bf16),
            pltpu.VMEM((kv_heads, 2, head_size, width), f32),
            pltpu.VMEM((kv_heads, 2, 1, width), f32),
            pltpu.VMEM((kv_heads, 2, 1, width), f32),
            pltpu.VMEM((tokens, query_heads * head_size), bf16),
            pltpu.VMEM((parts, tokens, slabs * slab), bf16),
            pltpu.VMEM((parts, tokens, slabs * slab), bf16),
            pltpu.VMEM((parts, tokens, slabs * slab), bf16),
            dma((5,)),
            dma((2, n)),
            dma((2, n)),
            dma((2, n)),
            dma((n,)),
            dma((n,)),
            dma((n,)),
            dma((n,)),
            dma((n,)),
            dma((n,)),
            dma((n,)),
            dma((1,)),
            dma((n,)),
            dma((n,)),
            dma((n,)),
            dma((n,)),
            dma((parts,)),
            dma((parts,)),
            dma((parts,)),
        ],
        compiler_params=pltpu.CompilerParams(
            collective_id=0, has_side_effects=True, vmem_limit_bytes=62 * 1024 * 1024
        ),
    )(query_states, key_states, value_rows, positions.reshape(2, half), out_weight)


def solution(mesh):
    n, groups = mesh.shape["ctx"], mesh.shape["groups"]
    row_stride = 1 << ((groups.bit_length() - 1) // 2)
    assert n % 4 == 0 and row_stride % 2 == 0 and groups % (2 * row_stride) == 0
    in_specs = (
        P(("groups", "ctx"), "tp", None),
        P(("groups", "ctx"), "tp", None),
        P(("groups", "ctx"), "tp", None),
        P(("groups", "ctx")),
        P("tp", "ctx"),
    )
    out_specs = P(("groups", "ctx"), "tp")
    return jax.shard_map(
        functools.partial(local, n, row_stride),
        mesh=mesh, in_specs=in_specs, out_specs=out_specs, check_vma=False,
    )
```

```python
import functools

import jax
import jax.numpy as jnp
from jax import lax
from jax.experimental import pallas as pl
from jax.experimental.pallas import tpu as pltpu
from jax.sharding import PartitionSpec as P

MESH = pl.DeviceIdType.MESH
LOG2E = 1.4426950408889634
LOW = -1e30
HIGH = 1e30
TAG_ROWS = 16
LANES = 1024
SLABS = 4


def flip(index, stride):
    return index + stride * (1 - 2 * lax.rem(index // stride, 2))


def kernel(
    n, row_stride, kv_heads, half, q_hbm, k_hbm, v_hbm, p_hbm, w_hbm, out_hbm,
    q_raw, k_raw, v_raw, p_raw, q_ref, kbuf, vbuf, wbuf, acc_ref, max_ref, sum_ref, att_ref, give_ref, take_ref, total_ref,
    in_sem, k_send, v_send, w_send, x_send, y_send, xd_send, yd_send,
    k_recv, v_recv, w_recv, w_last_recv, x_recv, y_recv, xd_recv, yd_recv, give_send, take_recv, out_sem,
):
    me, group, core = (lax.axis_index(a) for a in ("ctx", "groups", "tp"))
    head_size = q_ref.shape[2]
    width = q_ref.shape[3]
    chunks = width // LANES
    keys = 2 * half
    scale = LOG2E * head_size ** (-0.5)
    rows = wbuf.shape[1]
    quarter, eighth = rows // 4, rows // 8
    steps = n // 2

    right, left = lax.rem(me + 1, n), lax.rem(me + n - 1, n)
    x_group, y_group = flip(group, 1), flip(group, row_stride)
    px, py = lax.rem(group, 2), lax.rem(group // row_stride, 2)
    mine = pl.multiple_of((2 * py + px) * quarter, quarter)
    of_x = pl.multiple_of((2 * py + 1 - px) * quarter, quarter)
    of_y = pl.multiple_of((2 * (1 - py) + px) * quarter, quarter)
    of_xy = pl.multiple_of((2 * (1 - py) + 1 - px) * quarter, quarter)
    to_right, to_left = {"ctx": right}, {"ctx": left}
    to_x, to_y, to_twin = {"groups": x_group}, {"groups": y_group}, {"tp": 1 - core}

    def remote(ref, send, recv, device):
        return pltpu.make_async_remote_copy(
            src_ref=ref, dst_ref=ref, send_sem=send, recv_sem=recv, device_id=device, device_id_type=MESH
        )

    def way(d):
        return to_right if d == 0 else to_left

    def k_copy(d, slot):
        return remote(kbuf.at[slot], k_send.at[d, slot], k_recv.at[slot], way(d))

    def v_copy(d, slot):
        return remote(vbuf.at[slot], v_send.at[d, slot], v_recv.at[slot], way(d))

    def w_copy(d, slot):
        return remote(wbuf.at[slot, pl.ds(mine, quarter)], w_send.at[d, slot], w_recv.at[slot], way(d))

    def w_last_copy(d, slot):
        ref = wbuf.at[slot, pl.ds(mine + d * eighth, eighth)]
        return remote(ref, w_send.at[d, slot], w_recv.at[slot] if d == 0 else w_last_recv.at[0], way(d))

    def x_copy(slot, start):
        return remote(wbuf.at[slot, pl.ds(start, quarter)], x_send.at[slot], x_recv.at[slot], to_x)

    def y_copy(slot, start):
        return remote(wbuf.at[slot, pl.ds(start, quarter)], y_send.at[slot], y_recv.at[slot], to_y)

    def xd_copy(slot, start):
        return remote(wbuf.at[slot, pl.ds(start, eighth)], xd_send.at[slot], xd_recv.at[slot], to_x)

    def yd_copy(slot, start):
        return remote(wbuf.at[slot, pl.ds(start + eighth, eighth)], yd_send.at[slot], yd_recv.at[slot], to_y)

    def side(slot):
        x_copy(slot, mine).start()
        y_copy(slot, mine).start()

    def relay(slot):
        x_copy(slot, of_x).wait_recv()
        yd_copy(slot, of_x).start()
        y_copy(slot, of_y).wait_recv()
        xd_copy(slot, of_y).start()

    own = (
        pltpu.make_async_copy(w_hbm, wbuf.at[me], in_sem.at[0]),
        pltpu.make_async_copy(k_hbm, k_raw, in_sem.at[1]),
        pltpu.make_async_copy(p_hbm, p_raw, in_sem.at[2]),
        pltpu.make_async_copy(v_hbm, v_raw, in_sem.at[3]),
        pltpu.make_async_copy(q_hbm, q_raw, in_sem.at[4]),
    )
    for copy in own:
        copy.start()

    barrier = pltpu.get_barrier_semaphore()
    for device in (to_right, to_left, to_x, to_y, to_twin):
        pl.semaphore_signal(barrier, inc=1, device_id=device, device_id_type=MESH)
    pl.semaphore_wait(barrier, 5)

    own[0].wait()
    for d in (0, 1):
        w_copy(d, me).start()

    own[1].wait()
    own[2].wait()
    for kv in range(kv_heads):
        kbuf[me, kv * keys : (kv + 1) * keys, :] = k_raw[:, kv, :]
    place = p_raw[0:1, 0:1].astype(jnp.float32) / half
    kbuf[me, kv_heads * keys :, :] = jnp.broadcast_to(place, (TAG_ROWS, head_size)).astype(jnp.bfloat16)
    own[3].wait()
    for kv in range(kv_heads):
        vbuf[me, kv] = v_raw[:, kv, :].T
    for d in (0, 1):
        k_copy(d, me).start()

    own[4].wait()
    heads = width // half
    for kv in range(kv_heads):
        for h in range(heads):
            turned = q_raw[:, kv * heads + h, :].T
            for part in (0, 1):
                q_ref[kv, part, :, h * half : (h + 1) * half] = turned[:, part * half : (part + 1) * half]
        if kv == 0:
            for d in (0, 1):
                v_copy(d, me).start()

    def places(i):
        kv = i // chunks
        return kv, pl.ds(pl.multiple_of(lax.rem(i, chunks) * LANES, LANES), LANES)

    def scores_of(key_part, kv, part, lanes):
        return jnp.dot(key_part, q_ref[kv, part, :, lanes], preferred_element_type=jnp.float32)

    def powers(scores, shift):
        return jnp.exp2((scores - shift) * scale)

    def column_max(scores):
        return jnp.max(scores, axis=0, keepdims=True)

    def column_sum(values):
        return jnp.sum(values, axis=0, keepdims=True)

    def first(i, _):
        kv, lanes = places(i)
        key_rows = pl.multiple_of(kv * keys, keys)
        key_block = kbuf[me, pl.ds(key_rows, keys), :]
        values = vbuf[me, kv]
        shape = (half, LANES)
        tri = lax.broadcasted_iota(jnp.int32, shape, 0) <= lax.rem(lax.broadcasted_iota(jnp.int32, shape, 1), half)
        for part in (0, 1):
            scores = scores_of(key_block[: half * (part + 1)], kv, part, lanes)
            pieces = [scores[half * j : half * (j + 1)] for j in range(part + 1)]
            pieces[part] = jnp.where(tri, pieces[part], LOW)
            largest = functools.reduce(jnp.maximum, [column_max(p) for p in pieces])
            exps = jnp.concatenate([powers(p, largest) for p in pieces], axis=0)
            max_ref[kv, part, :, lanes] = largest
            sum_ref[kv, part, :, lanes] = column_sum(exps)
            acc_ref[kv, part, :, lanes] = jnp.dot(
                values[:, : half * (part + 1)], exps.astype(jnp.bfloat16), preferred_element_type=jnp.float32
            )
        return 0

    lax.fori_loop(0, kv_heads * chunks, first, 0)

    def tag(slot):
        row = kbuf[slot, kv_heads * keys :, :].astype(jnp.float32)[:1]
        return jnp.concatenate([row] * (LANES // row.shape[1]), axis=1)

    def attend(slot, kv):
        theirs, ours = tag(slot), tag(me)
        before, after = theirs < ours, theirs > ours

        def one(i, _):
            lanes = pl.ds(pl.multiple_of(i * LANES, LANES), LANES)
            key_rows = pl.multiple_of(kv * keys, keys)
            key_block = kbuf[slot, pl.ds(key_rows, keys), :]
            values = vbuf[slot, kv]

            def renew(part, largest, shifts, pieces, value_part):
                old = max_ref[kv, part, :, lanes]
                factor = jnp.exp2((old - largest) * scale)
                exps = jnp.concatenate([powers(p, s) for p, s in zip(pieces, shifts)], axis=0)
                max_ref[kv, part, :, lanes] = largest
                sum_ref[kv, part, :, lanes] = sum_ref[kv, part, :, lanes] * factor + column_sum(exps)
                acc_ref[kv, part, :, lanes] = acc_ref[kv, part, :, lanes] * factor + jnp.dot(
                    value_part, exps.astype(jnp.bfloat16), preferred_element_type=jnp.float32
                )

            low = scores_of(key_block[:half], kv, 0, lanes)
            largest = jnp.maximum(max_ref[kv, 0, :, lanes], jnp.where(before, column_max(low), LOW))
            renew(0, largest, [jnp.where(before, largest, HIGH)], [low], values[:, :half])

            high = scores_of(key_block, kv, 1, lanes)
            pieces = [high[:half], high[half:]]
            largest = jnp.maximum(column_max(pieces[0]), jnp.where(after, column_max(pieces[1]), LOW))
            largest = jnp.maximum(max_ref[kv, 1, :, lanes], largest)
            renew(1, largest, [largest, jnp.where(after, largest, HIGH)], pieces, values)
            return 0

        lax.fori_loop(0, chunks, one, 0)

    def attend_all(slot):
        def one(kv, _):
            attend(slot, kv)
            return 0

        lax.fori_loop(0, kv_heads, one, 0)

    def behind(s):
        return lax.rem(me + n - s, n)

    def ahead(s):
        return lax.rem(me + s, n)

    def arrived_at(slot):
        xd_copy(slot, of_xy).wait_recv()
        yd_copy(slot, of_xy).wait_recv()

    def arrived(s):
        arrived_at(behind(s))
        arrived_at(ahead(s))

    def sent_aside(slot):
        x_copy(slot, mine).wait_send()
        y_copy(slot, mine).wait_send()
        yd_copy(slot, of_x).wait_send()
        xd_copy(slot, of_y).wait_send()

    def sent(s):
        a, b = behind(s), ahead(s)
        k_copy(0, a).wait_send()
        v_copy(1, b).wait_send()

        @pl.when(s < steps - 1)
        def _():
            k_copy(1, b).wait_send()
            v_copy(0, a).wait_send()
            w_copy(0, a).wait_send()
            w_copy(1, b).wait_send()

        @pl.when(s == steps - 1)
        def _():
            w_last_copy(0, a).wait_send()
            w_last_copy(1, b).wait_send()

        sent_aside(a)
        sent_aside(b)

    def each(low, high, what):
        def one(s, _):
            what(s)
            return 0

        lax.fori_loop(max(low, 1), high, one, 0)

    def step(s, _):
        a, b = behind(s), ahead(s)
        w_copy(0, a).wait_recv()
        w_copy(1, b).wait_recv()

        @pl.when(s < steps - 1)
        def _():
            w_copy(0, a).start()
            w_copy(1, b).start()

        @pl.when(s == steps - 1)
        def _():
            w_last_copy(0, a).start()
            w_last_copy(1, b).start()

        side(a)
        side(b)

        @pl.when(s > 1)
        def _():
            attend(ahead(s - 1), 0)

        k_copy(0, a).wait_recv()
        k_copy(0, a).start()
        k_copy(1, b).wait_recv()

        @pl.when(s < steps - 1)
        def _():
            k_copy(1, b).start()

        @pl.when(s > 1)
        def _():
            relay(behind(s - 1))
            relay(ahead(s - 1))
            attend(ahead(s - 1), 1)

        v_copy(0, a).wait_recv()

        @pl.when(s < steps - 1)
        def _():
            v_copy(0, a).start()

        v_copy(1, b).wait_recv()
        v_copy(1, b).start()

        @pl.when(s > 2)
        def _():
            arrived(s - 2)

        @pl.when(s > 3)
        def _():
            sent(s - 3)

        attend_all(a)
        return 0

    lax.fori_loop(1, steps, step, 0)

    far = ahead(steps)
    w_last_copy(0, far).wait_recv()
    w_last_copy(1, far).wait_recv()
    side(far)
    attend_all(ahead(steps - 1))
    relay(behind(steps - 1))
    relay(ahead(steps - 1))
    k_copy(0, far).wait_recv()
    v_copy(1, far).wait_recv()
    attend_all(far)

    def finish(i, _):
        kv, part = i // 2, lax.rem(i, 2)
        for h in range(heads):
            lanes = slice(h * half, (h + 1) * half)
            tile = acc_ref[kv, part, :, lanes] * (1.0 / sum_ref[kv, part, :, lanes])
            columns = pl.ds(pl.multiple_of((kv * heads + h) * head_size, head_size), head_size)
            att_ref[pl.ds(pl.multiple_of(part * half, half), half), columns] = tile.T.astype(jnp.bfloat16)
        return 0

    lax.fori_loop(0, kv_heads * 2, finish, 0)

    relay(far)
    each(steps - 2, steps, arrived)

    parts = give_ref.shape[0]
    slabs = n // (2 * parts)
    span = give_ref.shape[2]
    far_part = lax.rem(far // slabs, parts)
    far_given = lax.rem(far // (slabs * parts) + core, 2)

    def turn(i):
        late = jnp.where(i < parts - 1, i, jnp.where(i < 2 * parts - 1, i + 1, parts - 1))
        turn = jnp.where(far_given == 1, late, i)
        return turn < parts, lax.rem(far_part + 1 + lax.rem(turn, parts), parts)

    def give_copy(part):
        return pltpu.make_async_remote_copy(
            src_ref=give_ref.at[part], dst_ref=take_ref.at[part], send_sem=give_send.at[part],
            recv_sem=take_recv.at[part], device_id=to_twin, device_id_type=MESH,
        )

    def out_copy(part):
        columns = pl.ds(pl.multiple_of(part * span, span), span)
        return pltpu.make_async_copy(total_ref.at[part], out_hbm.at[:, columns], out_sem.at[part])

    def pass_on(i):
        given, part = turn(i)

        @pl.when(given)
        def _():
            give_copy(part).start()

        @pl.when(jnp.logical_not(given))
        def _():
            out_copy(part).start()

    def project(i, _):
        given, part = turn(i)
        first_slab = slabs * (part + parts * jnp.where(given, 1 - core, core))

        @pl.when(i == 2 * parts - 1)
        def _():
            arrived_at(far)

        weight = jnp.concatenate([wbuf[first_slab + j] for j in range(slabs)], axis=1)
        product = jnp.dot(att_ref[...], weight, preferred_element_type=jnp.float32)

        @pl.when(i > 0)
        def _():
            pass_on(i - 1)

        @pl.when(given)
        def _():
            give_ref[part] = product.astype(jnp.bfloat16)

        @pl.when(jnp.logical_not(given))
        def _():
            give_copy(part).wait_recv()
            total_ref[part] = (product + take_ref[part].astype(jnp.float32)).astype(jnp.bfloat16)

        return 0

    lax.fori_loop(0, 2 * parts, project, 0)
    pass_on(2 * parts - 1)

    each(steps - 3, steps, sent)
    sent_aside(far)
    for d in (0, 1):
        for copy in (k_copy, v_copy, w_copy):
            copy(d, me).wait_send()
    for part in range(parts):
        give_copy(part).wait_send()
        out_copy(part).wait()


def local(n, row_stride, query_states, key_states, value_rows, positions, out_weight):
    tokens, query_heads, head_size = query_states.shape
    kv_heads = key_states.shape[1]
    heads = query_heads // kv_heads
    half = tokens // 2
    rows, slab = out_weight.shape
    parts = max(n // (2 * SLABS), 1)
    slabs = n // (2 * parts)
    width = heads * half
    dma, bf16, f32 = pltpu.SemaphoreType.DMA, jnp.bfloat16, jnp.float32
    anywhere = pl.BlockSpec(memory_space=pl.ANY)
    return pl.pallas_call(
        functools.partial(kernel, n, row_stride, kv_heads, half),
        out_shape=jax.ShapeDtypeStruct((tokens, n // 2 * slab), bf16),
        in_specs=[anywhere] * 5,
        out_specs=anywhere,
        scratch_shapes=[
            pltpu.VMEM(query_states.shape, bf16),
            pltpu.VMEM(key_states.shape, bf16),
            pltpu.VMEM(value_rows.shape, bf16),
            pltpu.VMEM((2, half), positions.dtype),
            pltpu.VMEM((kv_heads, 2, head_size, width), bf16),
            pltpu.VMEM((n, kv_heads * tokens + TAG_ROWS, head_size), bf16),
            pltpu.VMEM((n, kv_heads, head_size, tokens), bf16),
            pltpu.VMEM((n, rows, slab), bf16),
            pltpu.VMEM((kv_heads, 2, head_size, width), f32),
            pltpu.VMEM((kv_heads, 2, 1, width), f32),
            pltpu.VMEM((kv_heads, 2, 1, width), f32),
            pltpu.VMEM((tokens, query_heads * head_size), bf16),
            pltpu.VMEM((parts, tokens, slabs * slab), bf16),
            pltpu.VMEM((parts, tokens, slabs * slab), bf16),
            pltpu.VMEM((parts, tokens, slabs * slab), bf16),
            dma((5,)),
            dma((2, n)),
            dma((2, n)),
            dma((2, n)),
            dma((n,)),
            dma((n,)),
            dma((n,)),
            dma((n,)),
            dma((n,)),
            dma((n,)),
            dma((n,)),
            dma((1,)),
            dma((n,)),
            dma((n,)),
            dma((n,)),
            dma((n,)),
            dma((parts,)),
            dma((parts,)),
            dma((parts,)),
        ],
        compiler_params=pltpu.CompilerParams(
            collective_id=0, has_side_effects=True, vmem_limit_bytes=62 * 1024 * 1024
        ),
    )(query_states, key_states, value_rows, positions.reshape(2, half), out_weight)


def solution(mesh):
    n, groups = mesh.shape["ctx"], mesh.shape["groups"]
    row_stride = 1 << ((groups.bit_length() - 1) // 2)
    assert n % 4 == 0 and row_stride % 2 == 0 and groups % (2 * row_stride) == 0
    in_specs = (
        P(("groups", "ctx"), "tp", None),
        P(("groups", "ctx"), "tp", None),
        P(("groups", "ctx"), "tp", None),
        P(("groups", "ctx")),
        P("tp", "ctx"),
    )
    out_specs = P(("groups", "ctx"), "tp")
    return jax.shard_map(
        functools.partial(local, n, row_stride),
        mesh=mesh, in_specs=in_specs, out_specs=out_specs, check_vma=False,
    )
```
